32 devices in a mesh: pipe: 2 (over core), dp: 8 (over z, y), mp: 2 (over x).
Axes of the slice: x: 2, y: 2, z: 4, core: 2. Of those that a mesh axis runs over, the one named last changes fastest.
Arguments:
- token_ids: int32 [2, 4096], P('pipe', 'dp'), may hold values from 0 to 32127, as said below
- embedded: bfloat16 [2, 4096, 4096], P('pipe', 'dp', 'mp'), may hold values from -720 to 720
- norm_gain: float32 [2, 4096], P('pipe', 'mp'), may hold values from 0.25 to 1.75
- proj_grad: bfloat16 [2, 4096, 2048], P('pipe', 'dp'), may hold values from -6 to 6
- proj_weight: bfloat16 [2, 4096, 2048], P('pipe', 'mp'), may hold values from -0.125 to 0.125
- stream_grad: bfloat16 [2, 4096, 4096], P('pipe', 'dp', 'mp'), may hold values from -6 to 6
Outputs:
- table_grad: float32 [32128, 2, 2048], P('dp', 'mp', 'pipe')
The draws below stay inside these ranges and needn't reach their ends.
Inputs may be any that keep to these rules, and one draw needn't show every extreme that they name: `token_ids`: call block o the ids o * 4016 to (o + 1) * 4016 - 1. The 512 tokens of one stack on one index of dp hold at most 128 ids of any one block, and some block gets exactly 128 of them.
All inputs are finite; a program needn't handle non-finite values.
Results may differ from the reference program's by a relative error of at most 0.0029.
Values may be sent and summed in bfloat16 or wider, within the bound.
A program may use at most 128 MiB of HBM per device.

```python
import math
import jax
import jax.numpy as jnp
from jax import lax

D = 4096
VOCAB = 32128
INNER = 2048
TOK_DEV = 512
TOKENS = 4096
CAP = 128
VR = 4016
N_DP = 8


def draw_token_ids(key, part):
    hot_rows = jax.random.randint(jax.random.fold_in(key, 7), (N_DP,), 0, VR)

    def draw_block(section_number, replica):
        full_owner = jax.random.randint(jax.random.fold_in(jax.random.fold_in(key, 11), section_number), (), 0, N_DP)
        block_key = jax.random.fold_in(jax.random.fold_in(key, 101 + section_number), replica)
        key_slots, key_order, key_choose, key_rows = jax.random.split(block_key, 4)
        remaining = jax.random.permutation(key_slots, (N_DP - 1) * CAP)[:TOK_DEV - CAP]
        owners_rest = (remaining // CAP + full_owner + 1) % N_DP
        owners = jnp.concatenate([jnp.full((CAP,), full_owner, jnp.int32), owners_rest.astype(jnp.int32)])
        owners = owners[jax.random.permutation(key_order, TOK_DEV)]
        chooser = jax.random.randint(key_choose, (TOK_DEV,), 0, 4)
        uniform_rows = jax.random.randint(key_rows, (TOK_DEV,), 0, VR)
        picked = jnp.where(chooser == 0, hot_rows[owners], uniform_rows)
        return (owners * VR + picked).astype(jnp.int32)
    sections = jnp.arange(2, dtype=jnp.int32)
    replicas = jnp.arange(N_DP, dtype=jnp.int32)
    blocks = jax.vmap(lambda section_number: jax.vmap(lambda replica: draw_block(section_number, replica))(replicas))(sections)
    return blocks.reshape(2, TOKENS)


def draw_embedded(key, part):
    key_base, key_rows = jax.random.split(key, 2)
    columns = jnp.arange(D, dtype=jnp.float32) / (D - 1)
    base = jax.random.normal(key_base, (2 * TOKENS, D), jnp.float32)
    row_scale = jnp.exp(jax.random.uniform(key_rows, (2 * TOKENS, 1), jnp.float32, 0.0, math.log(10.0)))
    column_scale = jnp.exp(columns * math.log(3.0))
    base = jnp.clip(base, -5.0, 5.0)
    return (base * row_scale * column_scale[None, :]).astype(jnp.bfloat16).reshape(2, TOKENS, D)


def steps_of(rng, extent, cuts, smallest, largest):
    def one(dim, shards_of):
        draws = jax.random.uniform(jax.random.fold_in(jax.random.fold_in(rng, 6), dim), (shards_of,), jnp.float32, smallest / len(cuts), largest / len(cuts))
        return jnp.repeat(jnp.exp(draws), extent[dim] // shards_of).reshape((-1,) + (1,) * (len(extent) - dim - 1))

    factor_of = one(*cuts[0])
    for cut in cuts[1:]:
        factor_of = factor_of * one(*cut)
    return factor_of


def noise(own_key, shape, deviation, limit, shards=(), held_as=jnp.bfloat16):
    drawn = jax.random.normal(own_key, shape, jnp.float32) * deviation
    if len(shards) > 0:
        drawn = steps_of(own_key, shape, shards, -0.22, 0.18) * drawn
    return jnp.clip(drawn, min=-limit, max=limit).astype(held_as)


def setup_inputs(seed: int = 0) -> dict:
    key_of = jax.random.split(jax.random.key(seed), 7)
    token_ids = draw_token_ids(jax.random.fold_in(key_of[6], 71), 0)
    embedded = draw_embedded(jax.random.fold_in(key_of[6], 71), 0)
    norm_gain = jnp.clip(1.0 + 0.15 * jax.random.normal(key_of[2], (2, D), jnp.float32), 0.25, 1.75)
    proj_grad = noise(key_of[3], (2, TOKENS, INNER), 1.0, 6.0, ((0, 2), (1, 8)))
    proj_weight = noise(key_of[4], (2, D, INNER), INNER ** -0.5, 0.125, ((0, 2), (1, 2)))
    stream_grad = noise(key_of[5], (2, TOKENS, D), 1.0, 6.0, ((0, 2), (1, 8), (2, 2)))
    return dict(token_ids=token_ids, embedded=embedded, norm_gain=norm_gain, proj_grad=proj_grad, proj_weight=proj_weight, stream_grad=stream_grad)


epsilon = 1e-06

def stack_back(grad, weight, embed, gain, stream):
    query_back = jnp.dot(grad, weight.T, preferred_element_type=jnp.float32)
    inputs = embed.astype(jnp.float32)
    scaled = query_back * gain.astype(jnp.float32)[None, :]
    square_sum = lax.optimization_barrier(jnp.sum(inputs * inputs, axis=1))
    mixed_sum = lax.optimization_barrier(jnp.sum(inputs * scaled, axis=1))
    inverse = lax.rsqrt(square_sum / D + epsilon)
    norm_back = inverse[:, None] * scaled - inputs * (inverse * inverse * inverse * mixed_sum / D)[:, None]
    return (stream.astype(jnp.float32) + norm_back).astype(jnp.bfloat16)

def reference(token_ids, embedded, norm_gain, proj_grad, proj_weight, stream_grad):
    first = stack_back(proj_grad[0], proj_weight[0], embedded[0], norm_gain[0], stream_grad[0])
    second = stack_back(proj_grad[1], proj_weight[1], embedded[1], norm_gain[1], stream_grad[1])
    all_rows = jnp.concatenate([first, second], axis=0).astype(jnp.float32)
    table = jax.ops.segment_sum(all_rows, token_ids.reshape(-1).astype(jnp.int32), num_segments=VOCAB)
    return table.reshape(VOCAB, 2, D // 2)
```

```python
import functools

import jax
import jax.numpy as jnp
from jax import lax
from jax.experimental import pallas as pl
from jax.experimental.pallas import tpu as pltpu
from jax.sharding import PartitionSpec as P

VOCAB = 32128
LANES = 128
epsilon = 1e-06
VMEM_LIMIT = 60 * 1024 * 1024


def partner(me, k, n):
    out, bit = 0, 1
    while bit < n:
        mine = (me // bit) % 2
        flip = (k // bit) % 2
        out = out + bit * (mine + flip - 2 * mine * flip)
        bit *= 2
    return out


def contract_last(a, b):
    return lax.dot_general(a, b, (((1,), (1,)), ((), ())), preferred_element_type=jnp.float32)


def exchange_kernel(
    n, n_mp, cap, block_rows, full_width, chunk, token_chunk,
    ids_ref, gain_ref, embedded, proj_grad, weight, stream,
    rows_out, index_out,
    emb_v, grad_v, weight_v, stream_v, scaled_v, rows_v, send_v, sendi_v, sums_v, sums_got, position_v, local_v,
    in_sem, weight_sem, sum_send, sum_recv, send_sem, recv_sem, isend_sem, irecv_sem, own_sem,
):
    pipe = lax.axis_index("pipe")
    me = lax.axis_index("dp")
    mp = lax.axis_index("mp")
    other = 1 - pipe
    tokens, width = emb_v.shape
    half = width // 2

    loads = [
        pltpu.make_async_copy(proj_grad, grad_v, in_sem.at[0]),
        pltpu.make_async_copy(embedded, emb_v, in_sem.at[1]),
        pltpu.make_async_copy(stream, stream_v, in_sem.at[2]),
    ]
    chunks = [
        pltpu.make_async_copy(
            weight.at[pl.ds(j * chunk, chunk)], weight_v.at[pl.ds(j * chunk, chunk)], weight_sem.at[j]
        )
        for j in range(width // chunk)
    ]
    loads[0].start()
    chunks[0].start()
    loads[1].start()
    for copy in chunks[1:]:
        copy.start()
    loads[2].start()

    barrier = pltpu.get_barrier_semaphore()

    def greet(k, carry):
        d = partner(me, k, n)
        pl.semaphore_signal(
            barrier, inc=1, device_id={"dp": d, "pipe": other}, device_id_type=pl.DeviceIdType.MESH
        )

        @pl.when(k > 0)
        def _():
            pl.semaphore_signal(
                barrier, inc=1, device_id={"dp": d, "pipe": pipe}, device_id_type=pl.DeviceIdType.MESH
            )

        return carry

    lax.fori_loop(0, n, greet, 0)
    pl.semaphore_signal(
        barrier, inc=1, device_id={"mp": 1 - mp}, device_id_type=pl.DeviceIdType.MESH
    )

    ids = ids_ref[...]
    owner_low = lax.broadcasted_iota(jnp.int32, (n, tokens), 0) * block_rows
    match = (ids >= owner_low) & (ids < owner_low + block_rows)
    match_f = match.astype(jnp.float32)
    before = (
        lax.broadcasted_iota(jnp.int32, (tokens, tokens), 0)
        < lax.broadcasted_iota(jnp.int32, (tokens, tokens), 1)
    ).astype(jnp.float32).astype(jnp.bfloat16)
    rank = jnp.dot(match_f.astype(jnp.bfloat16), before, preferred_element_type=jnp.float32)
    slot_low = (lax.broadcasted_iota(jnp.int32, (n, tokens), 0) * cap).astype(jnp.float32)
    position_v[...] = jnp.sum(match_f * (slot_low + rank), axis=0, keepdims=True).astype(jnp.int32)
    local = ids - jnp.sum(jnp.where(match, owner_low, 0), axis=0, keepdims=True)
    high = local // 64
    row = lax.broadcasted_iota(jnp.int32, (8, tokens), 0)
    local_v[...] = (
        jnp.where(row == 0, high, jnp.where(row == 1, local - high * 64, 0))
        .astype(jnp.float32).astype(jnp.bfloat16)
    )

    loads[0].wait()
    mixed = jnp.zeros((tokens, 1), jnp.float32)
    square = jnp.zeros((tokens, 1), jnp.float32)
    for j in range(width // chunk):
        cols = pl.ds(j * chunk, chunk)
        chunks[j].wait()
        if j == 0:
            loads[1].wait()
        scaled = contract_last(grad_v[...], weight_v[cols, :]) * gain_ref[:, cols]
        scaled_v[:, cols] = scaled
        inputs = emb_v[:, cols].astype(jnp.float32)
        square = square + jnp.sum(inputs * inputs, axis=1, keepdims=True)
        mixed = mixed + jnp.sum(inputs * scaled, axis=1, keepdims=True)
    lane = lax.broadcasted_iota(jnp.int32, (tokens, LANES), 1)
    packed = jnp.where(lane == 0, square, jnp.where(lane == 1, mixed, 0.0))
    sums_v[...] = packed.T[:8]

    pl.semaphore_wait(barrier, 2 * n)
    swap = pltpu.make_async_remote_copy(
        src_ref=sums_v, dst_ref=sums_got, send_sem=sum_send, recv_sem=sum_recv,
        device_id={"mp": 1 - mp}, device_id_type=pl.DeviceIdType.MESH,
    )
    swap.start()

    def place_index(k, carry):
        d = partner(me, k, n)
        slots = d * cap + lax.broadcasted_iota(jnp.int32, (cap, tokens), 0)
        placer = (position_v[...] == slots).astype(jnp.float32).astype(jnp.bfloat16)
        parts = contract_last(local_v[...], placer)
        sendi_v[k] = (parts[0:1] * 64.0 + parts[1:2]).astype(jnp.int32)
        return carry

    lax.fori_loop(0, n, place_index, 0)
    loads[2].wait()
    swap.wait()

    total = sums_v[...] + sums_got[...]
    inverse = lax.rsqrt(total[0:1] / full_width + epsilon)
    coef = inverse * inverse * inverse * total[1:2] / full_width
    row8 = lax.broadcasted_iota(jnp.int32, (LANES, tokens), 0)
    back = jnp.where(row8 == 0, inverse, jnp.where(row8 == 1, coef, 0.0)).T
    sums_col_inv = back[:, 0:1]
    sums_col_coef = back[:, 1:2]
    for j in range(width // chunk):
        cols = pl.ds(j * chunk, chunk)
        norm_back = sums_col_inv * scaled_v[:, cols] - emb_v[:, cols].astype(jnp.float32) * sums_col_coef
        rows_v[:, cols] = (stream_v[:, cols].astype(jnp.float32) + norm_back).astype(jnp.bfloat16)

    def row_copy(k, p, d):
        return pltpu.make_async_remote_copy(
            src_ref=send_v.at[k, p], dst_ref=rows_out.at[k, pipe],
            send_sem=send_sem.at[k, p], recv_sem=recv_sem.at[k, pipe],
            device_id={"dp": d, "pipe": p}, device_id_type=pl.DeviceIdType.MESH,
        )

    def index_copy(k, p, d):
        return pltpu.make_async_remote_copy(
            src_ref=sendi_v.at[k], dst_ref=index_out.at[k, pipe],
            send_sem=isend_sem.at[k, p], recv_sem=irecv_sem.at[k, pipe],
            device_id={"dp": d, "pipe": p}, device_id_type=pl.DeviceIdType.MESH,
        )

    def send(k):
        d = partner(me, k, n)
        row_copy(k, other, d).start()
        index_copy(k, other, d).start()

        @pl.when(k > 0)
        def _():
            row_copy(k, pipe, d).start()
            index_copy(k, pipe, d).start()

    def place(k, carry):
        k = (k + 1) % n
        d = partner(me, k, n)
        slots = d * cap + lax.broadcasted_iota(jnp.int32, (cap, tokens), 0)
        placer = (position_v[...] == slots).astype(jnp.float32).astype(jnp.bfloat16)
        for p in range(2):
            send_v[k, p] = jnp.dot(
                placer, rows_v[:, p * half:(p + 1) * half], preferred_element_type=jnp.float32
            ).astype(jnp.bfloat16)

        @pl.when(k != 1 % n)
        def _():
            send((k + n - 1) % n)

        return carry

    lax.fori_loop(0, n, place, 0)
    send(0)
    own_rows = pltpu.make_async_copy(send_v.at[0, pipe], rows_out.at[0, pipe], own_sem.at[0])
    own_index = pltpu.make_async_copy(sendi_v.at[0], index_out.at[0, pipe], own_sem.at[1])
    own_rows.start()
    own_index.start()

    def arrive(k, carry):
        d = partner(me, k, n)
        for copy in (row_copy(k, other, d), index_copy(k, other, d)):
            copy.wait_send()

        @pl.when(k > 0)
        def _():
            for copy in (row_copy(k, pipe, d), index_copy(k, pipe, d)):
                copy.wait_send()

        for s_is_other in (True, False):
            s = other if s_is_other else pipe

            def wait_from():
                pltpu.make_async_remote_copy(
                    src_ref=send_v.at[k, pipe], dst_ref=rows_out.at[k, s],
                    send_sem=send_sem.at[k, pipe], recv_sem=recv_sem.at[k, s],
                    device_id={"dp": d, "pipe": other}, device_id_type=pl.DeviceIdType.MESH,
                ).wait_recv()
                pltpu.make_async_remote_copy(
                    src_ref=sendi_v.at[k], dst_ref=index_out.at[k, s],
                    send_sem=isend_sem.at[k, pipe], recv_sem=irecv_sem.at[k, s],
                    device_id={"dp": d, "pipe": other}, device_id_type=pl.DeviceIdType.MESH,
                ).wait_recv()

            if s_is_other:
                wait_from()
            else:
                pl.when(k > 0)(wait_from)
        return carry

    lax.fori_loop(0, n, arrive, 0)
    own_rows.wait()
    own_index.wait()


def exchange(ids, embedded, gain, proj_grad, weight, stream, n, n_mp, cap, block_rows):
    tokens, width = embedded.shape
    inner = proj_grad.shape[1]
    half = width // 2
    chunk = min(256, width)
    any_space = pl.BlockSpec(memory_space=pl.ANY)
    vmem = pl.BlockSpec(memory_space=pltpu.VMEM)
    dma = pltpu.SemaphoreType.DMA
    return pl.pallas_call(
        functools.partial(
            exchange_kernel, n, n_mp, cap, block_rows, width * n_mp, chunk, tokens
        ),
        out_shape=(
            jax.ShapeDtypeStruct((n, 2, cap, half), jnp.bfloat16),
            jax.ShapeDtypeStruct((n, 2, 1, cap), jnp.int32),
        ),
        in_specs=[vmem, vmem] + [any_space] * 4,
        out_specs=(any_space, any_space),
        scratch_shapes=[
            pltpu.VMEM((tokens, width), jnp.bfloat16),
            pltpu.VMEM((tokens, inner), jnp.bfloat16),
            pltpu.VMEM((width, inner), jnp.bfloat16),
            pltpu.VMEM((tokens, width), jnp.bfloat16),
            pltpu.VMEM((tokens, width), jnp.float32),
            pltpu.VMEM((tokens, width), jnp.bfloat16),
            pltpu.VMEM((n, 2, cap, half), jnp.bfloat16),
            pltpu.VMEM((n, 1, cap), jnp.int32),
            pltpu.VMEM((8, tokens), jnp.float32),
            pltpu.VMEM((8, tokens), jnp.float32),
            pltpu.VMEM((1, tokens), jnp.int32),
            pltpu.VMEM((8, tokens), jnp.bfloat16),
            dma((3,)),
            dma((width // chunk,)),
            dma,
            dma,
            dma((n, 2)),
            dma((n, 2)),
            dma((n, 2)),
            dma((n, 2)),
            dma((2,)),
        ],
        compiler_params=pltpu.CompilerParams(
            collective_id=0, has_side_effects=True, vmem_limit_bytes=VMEM_LIMIT
        ),
    )(ids, gain, embedded, proj_grad, weight, stream)


def table_kernel(cap, index_ref, rows_ref, out_ref, wide_v):
    lines = wide_v.shape[0] // cap
    blocks = rows_ref.shape[0]
    pieces = 16
    while out_ref.shape[0] % (8 * pieces):
        pieces //= 2
    zero_rows = out_ref.shape[0] // pieces

    def clear(i, carry):
        out_ref[pl.ds(pl.multiple_of(i * zero_rows, 8), zero_rows), :] = jnp.zeros(
            (zero_rows, LANES), jnp.float32
        )
        return carry

    lax.fori_loop(0, pieces, clear, 0)

    def block(b, carry):
        for j in range(lines):
            wide_v[pl.ds(j, cap, stride=lines), :] = rows_ref[b, :, j * LANES:(j + 1) * LANES].astype(
                jnp.float32
            )

        def add(g, carry):
            for u in range(8):
                c = g * 8 + u
                v = pl.multiple_of(index_ref[b, 0, c] * lines, lines)
                out_ref[pl.ds(v, lines), :] += wide_v[pl.ds(pl.multiple_of(c * lines, lines), lines), :]
            return carry

        return lax.fori_loop(0, cap // 8, add, carry)

    lax.fori_loop(0, blocks, block, 0)


def table(index, rows, block_rows):
    n, stacks, cap, half = rows.shape
    lines = half // LANES
    return pl.pallas_call(
        functools.partial(table_kernel, cap),
        out_shape=jax.ShapeDtypeStruct((block_rows * lines, LANES), jnp.float32),
        in_specs=[
            pl.BlockSpec(memory_space=pltpu.SMEM),
            pl.BlockSpec(memory_space=pltpu.VMEM),
        ],
        out_specs=pl.BlockSpec(memory_space=pltpu.VMEM),
        scratch_shapes=[pltpu.VMEM((cap * lines, LANES), jnp.float32)],
        compiler_params=pltpu.CompilerParams(vmem_limit_bytes=VMEM_LIMIT),
    )(index.reshape(n * stacks, 1, cap), rows.reshape(n * stacks, cap, half))


def on_device(token_ids, embedded, norm_gain, proj_grad, proj_weight, stream_grad):
    n = lax.axis_size("dp")
    tokens = token_ids.shape[1]
    cap = max(2, 2 * tokens // n)
    block_rows = VOCAB // n
    rows, index = exchange(
        token_ids, embedded[0], norm_gain, proj_grad[0], proj_weight[0], stream_grad[0],
        n, lax.axis_size("mp"), cap, block_rows,
    )
    half = rows.shape[-1]
    return table(index, rows, block_rows).reshape(block_rows, 1, half)


def solution(mesh):
    return jax.shard_map(
        on_device,
        mesh=mesh,
        in_specs=(
            P("pipe", "dp"),
            P("pipe", "dp", "mp"),
            P("pipe", "mp"),
            P("pipe", "dp", None),
            P("pipe", "mp", None),
            P("pipe", "dp", "mp"),
        ),
        out_specs=P("dp", "mp", "pipe"),
        check_vma=False,
    )
```

```python
import functools

import jax
import jax.numpy as jnp
from jax import lax
from jax.experimental import pallas as pl
from jax.experimental.pallas import tpu as pltpu
from jax.sharding import PartitionSpec as P

VOCAB = 32128
LANES = 128
epsilon = 1e-06
VMEM_LIMIT = 60 * 1024 * 1024


def partner(me, k, n):
    out, bit = 0, 1
    while bit < n:
        mine = (me // bit) % 2
        flip = (k // bit) % 2
        out = out + bit * (mine + flip - 2 * mine * flip)
        bit *= 2
    return out


def contract_last(a, b):
    return lax.dot_general(a, b, (((1,), (1,)), ((), ())), preferred_element_type=jnp.float32)


def greet_all(n, pipe, other, me, mp):
    barrier = pltpu.get_barrier_semaphore()

    def greet(k, carry):
        d = partner(me, k, n)
        pl.semaphore_signal(
            barrier, inc=1, device_id={"dp": d, "pipe": other}, device_id_type=pl.DeviceIdType.MESH
        )

        @pl.when(k > 0)
        def _():
            pl.semaphore_signal(
                barrier, inc=1, device_id={"dp": d, "pipe": pipe}, device_id_type=pl.DeviceIdType.MESH
            )

        return carry

    lax.fori_loop(0, n, greet, 0)
    if mp is not None:
        pl.semaphore_signal(
            barrier, inc=1, device_id={"mp": 1 - mp}, device_id_type=pl.DeviceIdType.MESH
        )
    return barrier


def find_places(n, cap, keep, spill, block_rows, ids_ref, position_v, local_v, spill_v, state_v):
    tokens = ids_ref.shape[1]
    ids = ids_ref[...]
    owner = lax.broadcasted_iota(jnp.int32, (n, tokens), 0)
    owner_low = owner * block_rows
    match = (ids >= owner_low) & (ids < owner_low + block_rows)
    match_f = match.astype(jnp.float32)
    before = (
        lax.broadcasted_iota(jnp.int32, (tokens, tokens), 0)
        < lax.broadcasted_iota(jnp.int32, (tokens, tokens), 1)
    ).astype(jnp.float32).astype(jnp.bfloat16)
    rank = match_f * jnp.dot(match_f.astype(jnp.bfloat16), before, preferred_element_type=jnp.float32)
    rank = jnp.sum(rank, axis=0, keepdims=True).astype(jnp.int32)
    token_owner = jnp.sum(jnp.where(match, owner, 0), axis=0, keepdims=True)
    position_v[...] = jnp.where(rank < keep, token_owner * cap + rank, -1)
    local = ids - token_owner * block_rows
    high = local // 64
    row = lax.broadcasted_iota(jnp.int32, (8, tokens), 0)
    parts = jnp.where(row == 0, high, jnp.where(row == 1, local - high * 64, 0))
    parts = jnp.where(row == 2, token_owner + 1, parts)
    local_v[...] = parts.astype(jnp.float32).astype(jnp.bfloat16)
    if spill:
        over = jnp.broadcast_to((rank >= keep).astype(jnp.float32), (8, tokens))
        over_rank = jnp.dot(over.astype(jnp.bfloat16), before, preferred_element_type=jnp.float32)
        spill_v[...] = jnp.where(rank >= keep, over_rank[0:1].astype(jnp.int32), -1)
        full = jnp.sum(over[0:1], axis=1, keepdims=True) > spill
        state_v[1:2, :] = jnp.broadcast_to(full.astype(jnp.float32), (1, LANES)).astype(jnp.int32)
        slots = lax.broadcasted_iota(jnp.int32, (LANES, tokens), 0)
        placer = (spill_v[...] == slots).astype(jnp.float32).astype(jnp.bfloat16)
        found = contract_last(local_v[...], placer)
        state_v[0:1, :] = (found[0:1] * 64.0 + found[1:2]).astype(jnp.int32)
        state_v[2:3, :] = found[2:3].astype(jnp.int32)


def place_indices(n, cap, keep, spill, me, position_v, local_v, state_v, sendi_v):
    tokens = position_v.shape[1]
    slots_here = LANES if spill else cap

    def place_index(k, carry):
        d = partner(me, k, n)
        slot = lax.broadcasted_iota(jnp.int32, (slots_here, tokens), 0)
        placer = (position_v[...] == d * cap + slot) & (slot < keep)
        placer = placer.astype(jnp.float32).astype(jnp.bfloat16)
        parts = contract_last(local_v[...], placer)
        primary = (parts[0:1] * 64.0 + parts[1:2]).astype(jnp.int32)
        if spill:
            sendi_v[k, :, 0:LANES] = primary
            mine = state_v[2:3, :] == d + 1
            lane = lax.broadcasted_iota(jnp.int32, (1, LANES), 1)
            count = jnp.sum((mine & (lane < spill)).astype(jnp.float32), axis=1, keepdims=True)
            sendi_v[k, :, LANES:2 * LANES] = jnp.where(mine, state_v[0:1, :], -1)
            sendi_v[k, :, 2 * LANES:] = jnp.where(lane == 0, state_v[1:2, :], count.astype(jnp.int32))
        else:
            sendi_v[k] = primary
        return carry

    lax.fori_loop(0, n, place_index, 0)


def place_rows(k, d, cap, keep, position_v, rows_v, send_v):
    tokens, width = rows_v.shape
    half = width // 2
    slots = d * cap + lax.broadcasted_iota(jnp.int32, (keep, tokens), 0)
    placer = (position_v[...] == slots).astype(jnp.float32).astype(jnp.bfloat16)
    for p in range(2):
        send_v[k, p] = jnp.dot(
            placer, rows_v[:, p * half:(p + 1) * half], preferred_element_type=jnp.float32
        ).astype(jnp.bfloat16)


def remote(src, dst, send_sem, recv_sem, **where):
    return pltpu.make_async_remote_copy(
        src_ref=src, dst_ref=dst, send_sem=send_sem, recv_sem=recv_sem,
        device_id=where, device_id_type=pl.DeviceIdType.MESH,
    )


def make_sender(n, pipe, other, me, send_v, sendi_v, rows_out, index_out, sems):
    send_sem, recv_sem, isend_sem, irecv_sem = sems

    def copies(k, p, s):
        d = partner(me, k, n)
        return (
            remote(send_v.at[k, p], rows_out.at[k, s], send_sem.at[k, p], recv_sem.at[k, s], dp=d, pipe=p),
            remote(sendi_v.at[k], index_out.at[k, s], isend_sem.at[k, p], irecv_sem.at[k, s], dp=d, pipe=p),
        )

    def send(k, own_chip):
        for copy in copies(k, other, pipe):
            copy.start()
        if not own_chip:
            for copy in copies(k, pipe, pipe):
                copy.start()

    def arrive(k, carry):
        for copy in copies(k, other, pipe):
            copy.wait_send()
        for copy in copies(k, other, other):
            copy.wait_recv()

        @pl.when(k > 0)
        def _():
            for copy in copies(k, pipe, pipe):
                copy.wait_send()
            for copy in copies(k, other, pipe):
                copy.wait_recv()

        return carry

    return send, arrive


def exchange_kernel(
    n, cap, keep, spill, block_rows, full_width, chunk,
    ids_ref, gain_ref, embedded, proj_grad, weight, stream,
    rows_out, index_out, spill_out, kept_out,
    emb_v, grad_v, weight_v, stream_v, scaled_v, rows_v, send_v, sendi_v, over_v, sums_v, sums_got,
    position_v, local_v, spill_v, state_v,
    in_sem, weight_sem, sum_send, sum_recv, send_sem, recv_sem, isend_sem, irecv_sem, own_sem,
    pair_send, pair_recv, line_send, line_recv, side_send, side_recv,
):
    pipe = lax.axis_index("pipe")
    me = lax.axis_index("dp")
    mp = lax.axis_index("mp")
    other = 1 - pipe
    tokens, width = emb_v.shape
    half = width // 2

    loads = [
        pltpu.make_async_copy(proj_grad, grad_v, in_sem.at[0]),
        pltpu.make_async_copy(embedded, emb_v, in_sem.at[1]),
        pltpu.make_async_copy(stream, stream_v, in_sem.at[2]),
    ]
    chunks = [
        pltpu.make_async_copy(
            weight.at[pl.ds(j * chunk, chunk)], weight_v.at[pl.ds(j * chunk, chunk)], weight_sem.at[j]
        )
        for j in range(width // chunk)
    ]
    loads[0].start()
    chunks[0].start()
    loads[1].start()
    for copy in chunks[1:]:
        copy.start()
    loads[2].start()
    barrier = greet_all(n, pipe, other, me, mp)
    find_places(n, cap, keep, spill, block_rows, ids_ref, position_v, local_v, spill_v, state_v)

    loads[0].wait()
    mixed = jnp.zeros((tokens, 1), jnp.float32)
    square = jnp.zeros((tokens, 1), jnp.float32)
    for j in range(width // chunk):
        cols = pl.ds(j * chunk, chunk)
        chunks[j].wait()
        if j == 0:
            loads[1].wait()
        scaled = contract_last(grad_v[...], weight_v[cols, :]) * gain_ref[:, cols]
        scaled_v[:, cols] = scaled
        inputs = emb_v[:, cols].astype(jnp.float32)
        square = square + jnp.sum(inputs * inputs, axis=1, keepdims=True)
        mixed = mixed + jnp.sum(inputs * scaled, axis=1, keepdims=True)
    lane = lax.broadcasted_iota(jnp.int32, (tokens, LANES), 1)
    packed = jnp.where(lane == 0, square, jnp.where(lane == 1, mixed, 0.0))
    sums_v[...] = packed.T[:8]

    pl.semaphore_wait(barrier, 2 * n)
    swap = remote(sums_v, sums_got, sum_send, sum_recv, mp=1 - mp)
    swap.start()
    place_indices(n, cap, keep, spill, me, position_v, local_v, state_v, sendi_v)
    loads[2].wait()
    swap.wait()

    total = sums_v[...] + sums_got[...]
    inverse = lax.rsqrt(total[0:1] / full_width + epsilon)
    coef = inverse * inverse * inverse * total[1:2] / full_width
    line = lax.broadcasted_iota(jnp.int32, (LANES, tokens), 0)
    back = jnp.where(line == 0, inverse, jnp.where(line == 1, coef, 0.0)).T
    for j in range(width // chunk):
        cols = pl.ds(j * chunk, chunk)
        norm_back = back[:, 0:1] * scaled_v[:, cols] - emb_v[:, cols].astype(jnp.float32) * back[:, 1:2]
        rows_v[:, cols] = (stream_v[:, cols].astype(jnp.float32) + norm_back).astype(jnp.bfloat16)

    send, arrive = make_sender(
        n, pipe, other, me, send_v, sendi_v, rows_out, index_out,
        (send_sem, recv_sem, isend_sem, irecv_sem),
    )
    if spill:
        slots = lax.broadcasted_iota(jnp.int32, (spill, tokens), 0)
        placer = (spill_v[...] == slots).astype(jnp.float32).astype(jnp.bfloat16)
        for p in range(2):
            over_v[p] = jnp.dot(
                placer, rows_v[:, p * half:(p + 1) * half], preferred_element_type=jnp.float32
            ).astype(jnp.bfloat16)
    place_rows(1, partner(me, 1, n), cap, keep, position_v, rows_v, send_v)
    rounds = []
    if spill:
        lines = n // 2
        at, beside = me // 2, partner(me, 1, n)
        pair = remote(over_v.at[other], spill_out.at[0, pipe], pair_send, pair_recv, pipe=other)
        pair.start()
        own_over = pltpu.make_async_copy(over_v.at[pipe], spill_out.at[0, pipe], own_sem.at[2])
        own_over.start()
        kept = pltpu.make_async_copy(rows_v, kept_out, own_sem.at[3])
        kept.start()

        def along(up, r, source, to):
            return remote(
                spill_out.at[partner(me, source, n)], spill_out.at[partner(to, source, n)],
                line_send.at[up, r], line_recv.at[up, r], dp=to,
            )

        def across(source):
            return remote(
                spill_out.at[partner(me, source, n)], spill_out.at[partner(beside, source, n)],
                side_send.at[source // 2], side_recv.at[source // 2], dp=beside,
            )

        def pass_on(r):
            for up in (1, 0):
                step = 2 if up else -2
                source = me - step * r
                here = (at >= r) if up else (at + r < lines)
                more = (at + 1 < lines) if up else (at >= 1)
                if r > 0:

                    @pl.when(here)
                    def _():
                        remote(
                            spill_out.at[0], spill_out.at[partner(me, source, n)],
                            line_send.at[up, r], line_recv.at[up, r], dp=beside,
                        ).wait_recv()
                        across(source).start()

                @pl.when(here & more)
                def _():
                    along(up, r + 1, source, me + step).start()

            if r == 0:
                across(me).start()

        def finish(r):
            for up in (1, 0):
                step = 2 if up else -2
                source = me - step * r
                here = (at >= r) if up else (at + r < lines)
                more = (at + 1 < lines) if up else (at >= 1)

                @pl.when(here & more)
                def _():
                    along(up, r + 1, source, me + step).wait_send()

        place_rows(2, partner(me, 2, n), cap, keep, position_v, rows_v, send_v)
        send(1, False)
        own_over.wait()
        pair.wait()
        pass_on(0)
        place_rows(3, partner(me, 3, n), cap, keep, position_v, rows_v, send_v)
        send(2, False)
        for k in range(4, n + 1):
            k_now = k % n
            place_rows(k_now, partner(me, k_now, n), cap, keep, position_v, rows_v, send_v)
            send(k - 1, False)
            if k % 2 == 0 and (k - 2) // 2 < lines:
                pass_on((k - 2) // 2)
                rounds.append((k - 2) // 2)
        send(0, True)
        for r in range(1, lines):
            if r not in rounds:
                pass_on(r)
    else:

        def place(k, carry):
            now = k % n
            place_rows(now, partner(me, now, n), cap, keep, position_v, rows_v, send_v)
            send(k - 1, False)
            return carry

        lax.fori_loop(2, n + 1, place, 0)
        send(0, True)
    own_rows = pltpu.make_async_copy(send_v.at[0, pipe], rows_out.at[0, pipe], own_sem.at[0])
    own_index = pltpu.make_async_copy(sendi_v.at[0], index_out.at[0, pipe], own_sem.at[1])
    own_rows.start()
    own_index.start()
    lax.fori_loop(0, n, arrive, 0)
    own_rows.wait()
    own_index.wait()
    if spill:
        for r in range(lines):
            finish(r)

        def side(z, carry):
            remote(
                spill_out.at[partner(me, 2 * z, n)], spill_out.at[partner(me, 2 * z + beside % 2, n)],
                side_send.at[z], side_recv.at[z], dp=beside,
            ).wait()
            return carry

        lax.fori_loop(0, lines, side, 0)
        kept.wait()


def exchange(ids, embedded, gain, proj_grad, weight, stream, n, n_mp, cap, keep, spill, block_rows):
    tokens, width = embedded.shape
    inner = proj_grad.shape[1]
    half = width // 2
    chunk = min(256, width)
    index_width = 3 * LANES if spill else cap
    over = (spill or 16, half)
    kept = (tokens, width) if spill else (8, LANES)
    any_space = pl.BlockSpec(memory_space=pl.ANY)
    vmem = pl.BlockSpec(memory_space=pltpu.VMEM)
    dma = pltpu.SemaphoreType.DMA
    return pl.pallas_call(
        functools.partial(exchange_kernel, n, cap, keep, spill, block_rows, width * n_mp, chunk),
        out_shape=(
            jax.ShapeDtypeStruct((n, 2, keep, half), jnp.bfloat16),
            jax.ShapeDtypeStruct((n, 2, 1, index_width), jnp.int32),
            jax.ShapeDtypeStruct((n if spill else 1, 2) + over, jnp.bfloat16),
            jax.ShapeDtypeStruct(kept, jnp.bfloat16),
        ),
        in_specs=[vmem, vmem] + [any_space] * 4,
        out_specs=(any_space,) * 4,
        scratch_shapes=[
            pltpu.VMEM((tokens, width), jnp.bfloat16),
            pltpu.VMEM((tokens, inner), jnp.bfloat16),
            pltpu.VMEM((width, inner), jnp.bfloat16),
            pltpu.VMEM((tokens, width), jnp.bfloat16),
            pltpu.VMEM((tokens, width), jnp.float32),
            pltpu.VMEM((tokens, width), jnp.bfloat16),
            pltpu.VMEM((n, 2, keep, half), jnp.bfloat16),
            pltpu.VMEM((n, 1, index_width), jnp.int32),
            pltpu.VMEM((2,) + over, jnp.bfloat16),
            pltpu.VMEM((8, tokens), jnp.float32),
            pltpu.VMEM((8, tokens), jnp.float32),
            pltpu.VMEM((1, tokens), jnp.int32),
            pltpu.VMEM((8, tokens), jnp.bfloat16),
            pltpu.VMEM((1, tokens), jnp.int32),
            pltpu.VMEM((8, LANES), jnp.int32),
            dma((3,)),
            dma((width // chunk,)),
            dma,
            dma,
            dma((n, 2)),
            dma((n, 2)),
            dma((n, 2)),
            dma((n, 2)),
            dma((4,)),
            dma,
            dma,
            dma((2, n)),
            dma((2, n)),
            dma((n,)),
            dma((n,)),
        ],
        compiler_params=pltpu.CompilerParams(
            collective_id=0, has_side_effects=True, vmem_limit_bytes=VMEM_LIMIT
        ),
    )(ids, gain, embedded, proj_grad, weight, stream)


def full_kernel(
    n, cap, block_rows, ids_ref, rows_v, rows_out, index_out, send_v, sendi_v, position_v, local_v,
    send_sem, recv_sem, isend_sem, irecv_sem, own_sem,
):
    pipe = lax.axis_index("pipe")
    me = lax.axis_index("dp")
    other = 1 - pipe
    barrier = greet_all(n, pipe, other, me, None)
    pl.semaphore_wait(barrier, 2 * n - 1)
    find_places(n, cap, cap, 0, block_rows, ids_ref, position_v, local_v, None, None)
    place_indices(n, cap, cap, 0, me, position_v, local_v, None, sendi_v)
    send, arrive = make_sender(
        n, pipe, other, me, send_v, sendi_v, rows_out, index_out,
        (send_sem, recv_sem, isend_sem, irecv_sem),
    )
    place_rows(1, partner(me, 1, n), cap, cap, position_v, rows_v, send_v)

    def place(k, carry):
        now = k % n
        place_rows(now, partner(me, now, n), cap, cap, position_v, rows_v, send_v)
        send(k - 1, False)
        return carry

    lax.fori_loop(2, n + 1, place, 0)
    send(0, True)
    own_rows = pltpu.make_async_copy(send_v.at[0, pipe], rows_out.at[0, pipe], own_sem.at[0])
    own_index = pltpu.make_async_copy(sendi_v.at[0], index_out.at[0, pipe], own_sem.at[1])
    own_rows.start()
    own_index.start()
    lax.fori_loop(0, n, arrive, 0)
    own_rows.wait()
    own_index.wait()


def full_exchange(ids, rows, n, cap, block_rows):
    tokens, width = rows.shape
    half = width // 2
    any_space = pl.BlockSpec(memory_space=pl.ANY)
    vmem = pl.BlockSpec(memory_space=pltpu.VMEM)
    dma = pltpu.SemaphoreType.DMA
    return pl.pallas_call(
        functools.partial(full_kernel, n, cap, block_rows),
        out_shape=(
            jax.ShapeDtypeStruct((n, 2, cap, half), jnp.bfloat16),
            jax.ShapeDtypeStruct((n, 2, 1, cap), jnp.int32),
        ),
        in_specs=[vmem, vmem],
        out_specs=(any_space, any_space),
        scratch_shapes=[
            pltpu.VMEM((n, 2, cap, half), jnp.bfloat16),
            pltpu.VMEM((n, 1, cap), jnp.int32),
            pltpu.VMEM((1, tokens), jnp.int32),
            pltpu.VMEM((8, tokens), jnp.bfloat16),
            dma((n, 2)),
            dma((n, 2)),
            dma((n, 2)),
            dma((n, 2)),
            dma((2,)),
        ],
        compiler_params=pltpu.CompilerParams(
            collective_id=1, has_side_effects=True, vmem_limit_bytes=VMEM_LIMIT
        ),
    )(ids, rows)


def table_kernel(spilled, index_ref, rows_ref, *rest):
    if spilled:
        over_ref, out_ref, wide_v, over_v, over_sem = rest
    else:
        out_ref, wide_v = rest
    blocks, cap, half = rows_ref.shape
    lines = half // LANES
    pieces = 16
    while out_ref.shape[0] % (8 * pieces):
        pieces //= 2
    zero_rows = out_ref.shape[0] // pieces

    def clear(i, carry):
        out_ref[pl.ds(pl.multiple_of(i * zero_rows, 8), zero_rows), :] = jnp.zeros(
            (zero_rows, LANES), jnp.float32
        )
        return carry

    lax.fori_loop(0, pieces, clear, 0)

    def add_row(v, c):
        v = pl.multiple_of(v * lines, lines)
        out_ref[pl.ds(v, lines), :] += wide_v[pl.ds(pl.multiple_of(c * lines, lines), lines), :]

    def block(b, carry):
        for j in range(lines):
            wide_v[pl.ds(j, cap, stride=lines), :] = rows_ref[b, :, j * LANES:(j + 1) * LANES].astype(
                jnp.float32
            )

        def add(g, carry):
            for u in range(8):
                add_row(index_ref[b, 0, g * 8 + u], g * 8 + u)
            return carry

        lax.fori_loop(0, cap // 8, add, 0)
        if spilled:

            @pl.when(index_ref[b, 0, 2 * LANES + 1] > 0)
            def _():
                fetch = pltpu.make_async_copy(over_ref.at[b], over_v, over_sem)
                fetch.start()
                fetch.wait()
                for j in range(lines):
                    wide_v[pl.ds(j, spilled, stride=lines), :] = over_v[:, j * LANES:(j + 1) * LANES].astype(
                        jnp.float32
                    )

                def add_spilled(c, carry):
                    v = index_ref[b, 0, LANES + c]

                    @pl.when(v >= 0)
                    def _():
                        add_row(v, c)

                    return carry

                lax.fori_loop(0, spilled, add_spilled, 0)

        return carry

    lax.fori_loop(0, blocks, block, 0)


def table(index, rows, over, block_rows):
    n, stacks, cap, half = rows.shape
    lines = half // LANES
    spilled = 0 if over is None else over.shape[2]
    operands = [index.reshape(n * stacks, 1, -1), rows.reshape(n * stacks, cap, half)]
    in_specs = [pl.BlockSpec(memory_space=pltpu.SMEM), pl.BlockSpec(memory_space=pltpu.VMEM)]
    scratch = [pltpu.VMEM((max(cap, spilled) * lines, LANES), jnp.float32)]
    if spilled:
        operands.append(over.reshape(n * stacks, spilled, half))
        in_specs.append(pl.BlockSpec(memory_space=pl.ANY))
        scratch += [pltpu.VMEM((spilled, half), jnp.bfloat16), pltpu.SemaphoreType.DMA]
    return pl.pallas_call(
        functools.partial(table_kernel, spilled),
        out_shape=jax.ShapeDtypeStruct((block_rows * lines, LANES), jnp.float32),
        in_specs=in_specs,
        out_specs=pl.BlockSpec(memory_space=pltpu.VMEM),
        scratch_shapes=scratch,
        compiler_params=pltpu.CompilerParams(vmem_limit_bytes=VMEM_LIMIT),
    )(*operands)


def on_device(token_ids, embedded, norm_gain, proj_grad, proj_weight, stream_grad):
    n = lax.axis_size("dp")
    tokens = token_ids.shape[1]
    cap = max(2, 2 * tokens // n)
    block_rows = VOCAB // n
    tiers = cap % 32 == 0 and cap <= LANES
    keep = cap // 2 if tiers else cap
    spill = keep + 16 if tiers else 0
    rows, index, over, kept = exchange(
        token_ids, embedded[0], norm_gain, proj_grad[0], proj_weight[0], stream_grad[0],
        n, lax.axis_size("mp"), cap, keep, spill, block_rows,
    )
    half = rows.shape[-1]
    if tiers:

        def whole():
            full_rows, full_index = full_exchange(token_ids, kept, n, cap, block_rows)
            return table(full_index, full_rows, None, block_rows)

        def short():
            return table(index, rows, over, block_rows)

        out = lax.cond(jnp.max(index[:, :, 0, 2 * LANES]) > 0, whole, short)
    else:
        out = table(index, rows, None, block_rows)
    return out.reshape(block_rows, 1, half)


def solution(mesh):
    return jax.shard_map(
        on_device,
        mesh=mesh,
        in_specs=(
            P("pipe", "dp"),
            P("pipe", "dp", "mp"),
            P("pipe", "mp"),
            P("pipe", "dp", None),
            P("pipe", "mp", None),
            P("pipe", "dp", "mp"),
        ),
        out_specs=P("dp", "mp", "pipe"),
        check_vma=False,
    )
```

```python
import functools

import jax
import jax.numpy as jnp
from jax import lax
from jax.experimental import pallas as pl
from jax.experimental.pallas import tpu as pltpu
from jax.sharding import PartitionSpec as P

VOCAB = 32128
LANES = 128
epsilon = 1e-06
VMEM_LIMIT = 60 * 1024 * 1024


def partner(me, k, n):
    out, bit = 0, 1
    while bit < n:
        mine = (me // bit) % 2
        flip = (k // bit) % 2
        out = out + bit * (mine + flip - 2 * mine * flip)
        bit *= 2
    return out


def contract_last(a, b):
    return lax.dot_general(a, b, (((1,), (1,)), ((), ())), preferred_element_type=jnp.float32)


def greet_all(n, pipe, other, me, mp):
    barrier = pltpu.get_barrier_semaphore()

    def greet(k, carry):
        d = partner(me, k, n)
        pl.semaphore_signal(
            barrier, inc=1, device_id={"dp": d, "pipe": other}, device_id_type=pl.DeviceIdType.MESH
        )

        @pl.when(k > 0)
        def _():
            pl.semaphore_signal(
                barrier, inc=1, device_id={"dp": d, "pipe": pipe}, device_id_type=pl.DeviceIdType.MESH
            )

        return carry

    lax.fori_loop(0, n, greet, 0)
    if mp is not None:
        pl.semaphore_signal(
            barrier, inc=1, device_id={"mp": 1 - mp}, device_id_type=pl.DeviceIdType.MESH
        )
    return barrier


def find_places(n, keep, spill, block_rows, me, ids_ref, placer_v, local_v, state_v):
    tokens = ids_ref.shape[1]
    ids = ids_ref[...]
    owner = lax.broadcasted_iota(jnp.int32, (n, tokens), 0)
    owner_low = owner * block_rows
    match = (ids >= owner_low) & (ids < owner_low + block_rows)
    match_f = match.astype(jnp.float32)
    before = (
        lax.broadcasted_iota(jnp.int32, (tokens, tokens), 0)
        < lax.broadcasted_iota(jnp.int32, (tokens, tokens), 1)
    ).astype(jnp.float32).astype(jnp.bfloat16)
    rank = match_f * jnp.dot(match_f.astype(jnp.bfloat16), before, preferred_element_type=jnp.float32)
    rank = jnp.sum(rank, axis=0, keepdims=True).astype(jnp.int32)
    token_owner = jnp.sum(jnp.where(match, owner, 0), axis=0, keepdims=True)
    position = jnp.where(rank < keep, partner(me, token_owner, n) * keep + rank, -1)
    local = ids - token_owner * block_rows
    high = local // 64
    row = lax.broadcasted_iota(jnp.int32, (8, tokens), 0)
    parts = jnp.where(row == 0, high, jnp.where(row == 1, local - high * 64, 0))
    parts = jnp.where(row == 2, token_owner + 1, parts)
    local_v[...] = parts.astype(jnp.float32).astype(jnp.bfloat16)
    if spill:
        over = match_f * (rank >= keep).astype(jnp.float32)
        count = jnp.sum(over, axis=1, keepdims=True)
        start = jnp.zeros((1, 1), jnp.float32)
        begin = jnp.zeros((1, tokens), jnp.float32)
        for o in range(n):
            begin = begin + over[o:o + 1] * start
            start = start + count[o:o + 1]
        behind = n * keep + begin.astype(jnp.int32) + rank - keep
        position = jnp.where(rank >= keep, behind, position)
        full = (start > spill).astype(jnp.float32)
        state_v[1:2, :] = jnp.broadcast_to(full, (1, LANES)).astype(jnp.int32)
    slots = lax.broadcasted_iota(jnp.int32, placer_v.shape, 0)
    placer_v[...] = (position == slots).astype(jnp.float32).astype(jnp.bfloat16)


def place_indices(n, keep, spill, me, placer_v, local_v, state_v, sendi_v):
    parts = contract_last(local_v[...], placer_v[...])
    found = (parts[0:1] * 64.0 + parts[1:2]).astype(jnp.int32)
    if spill:
        state_v[0:1, :] = found[:, n * keep:]
        state_v[2:3, :] = parts[2:3, n * keep:].astype(jnp.int32)
        lane = lax.broadcasted_iota(jnp.int32, (1, LANES), 1)
        sendi_v[...] = jnp.zeros(sendi_v.shape, jnp.int32)
    for k in range(n):
        sendi_v[k, :, 0:keep] = found[:, k * keep:(k + 1) * keep]
        if spill:
            d = partner(me, k, n)
            there = state_v[2:3, :]
            count = jnp.sum(((there == d + 1) & (lane < spill)).astype(jnp.float32), axis=1, keepdims=True)
            start = jnp.sum(((there > 0) & (there < d + 1)).astype(jnp.float32), axis=1, keepdims=True)
            facts = jnp.where(lane == 1, count, start).astype(jnp.int32)
            sendi_v[k, :, LANES:2 * LANES] = state_v[0:1, :]
            sendi_v[k, :, 2 * LANES:] = jnp.where(lane == 0, state_v[1:2, :], facts)


def place_rows(c, chunk, keep, spill, placer_v, part, send_v, over_v):
    n, _, _, half = send_v.shape
    p, cols = c * chunk // half, pl.ds(c * chunk % half, chunk)
    placed = jnp.dot(
        placer_v[0:n * keep + spill, :], part, preferred_element_type=jnp.float32
    ).astype(jnp.bfloat16)
    send_v[:, p, :, cols] = placed[:n * keep].reshape(n, keep, chunk)
    if spill:
        over_v[p, :, cols] = placed[n * keep:]


def remote(src, dst, send_sem, recv_sem, **where):
    return pltpu.make_async_remote_copy(
        src_ref=src, dst_ref=dst, send_sem=send_sem, recv_sem=recv_sem,
        device_id=where, device_id_type=pl.DeviceIdType.MESH,
    )


def make_sender(n, pipe, other, me, send_v, sendi_v, rows_out, index_out, sems):
    send_sem, recv_sem, isend_sem, irecv_sem = sems

    def copies(k, p, s):
        d = partner(me, k, n)
        return (
            remote(send_v.at[k, p], rows_out.at[k, s], send_sem.at[k, p], recv_sem.at[k, s], dp=d, pipe=p),
            remote(sendi_v.at[k], index_out.at[k, s], isend_sem.at[k, p], irecv_sem.at[k, s], dp=d, pipe=p),
        )

    def send(k, own_chip):
        for copy in copies(k, other, pipe):
            copy.start()
        if not own_chip:
            for copy in copies(k, pipe, pipe):
                copy.start()

    def arrive(k, carry):
        for copy in copies(k, other, pipe):
            copy.wait_send()
        for copy in copies(k, other, other):
            copy.wait_recv()

        @pl.when(k > 0)
        def _():
            for copy in copies(k, pipe, pipe):
                copy.wait_send()
            for copy in copies(k, other, pipe):
                copy.wait_recv()

        return carry

    return send, arrive


def exchange_kernel(
    n, cap, keep, spill, block_rows, full_width, chunk,
    ids_ref, gain_ref, embedded, proj_grad, weight, stream,
    rows_out, index_out, spill_out, kept_out,
    emb_v, grad_v, weight_v, stream_v, scaled_v, rows_v, send_v, sendi_v, over_v, sums_v, sums_got,
    placer_v, local_v, state_v,
    in_sem, weight_sem, sum_send, sum_recv, send_sem, recv_sem, isend_sem, irecv_sem, own_sem,
    pair_send, pair_recv, line_send, line_recv, side_send, side_recv,
):
    pipe = lax.axis_index("pipe")
    me = lax.axis_index("dp")
    mp = lax.axis_index("mp")
    other = 1 - pipe
    tokens, width = emb_v.shape
    half = width // 2

    loads = [
        pltpu.make_async_copy(proj_grad, grad_v, in_sem.at[0]),
        pltpu.make_async_copy(embedded, emb_v, in_sem.at[1]),
        pltpu.make_async_copy(stream, stream_v, in_sem.at[2]),
    ]
    chunks = [
        pltpu.make_async_copy(
            weight.at[pl.ds(j * chunk, chunk)], weight_v.at[pl.ds(j * chunk, chunk)], weight_sem.at[j]
        )
        for j in range(width // chunk)
    ]
    loads[0].start()
    chunks[0].start()
    loads[1].start()
    for copy in chunks[1:]:
        copy.start()
    loads[2].start()
    barrier = greet_all(n, pipe, other, me, mp)
    find_places(n, keep, spill, block_rows, me, ids_ref, placer_v, local_v, state_v)

    loads[0].wait()
    mixed = jnp.zeros((tokens, 1), jnp.float32)
    square = jnp.zeros((tokens, 1), jnp.float32)
    for j in range(width // chunk):
        cols = pl.ds(j * chunk, chunk)
        chunks[j].wait()
        if j == 0:
            loads[1].wait()
        scaled = contract_last(grad_v[...], weight_v[cols, :]) * gain_ref[:, cols]
        scaled_v[:, cols] = scaled
        inputs = emb_v[:, cols].astype(jnp.float32)
        square = square + jnp.sum(inputs * inputs, axis=1, keepdims=True)
        mixed = mixed + jnp.sum(inputs * scaled, axis=1, keepdims=True)
    lane = lax.broadcasted_iota(jnp.int32, (tokens, LANES), 1)
    packed = jnp.where(lane == 0, square, jnp.where(lane == 1, mixed, 0.0))
    sums_v[...] = packed.T[:8]

    pl.semaphore_wait(barrier, 2 * n)
    swap = remote(sums_v, sums_got, sum_send, sum_recv, mp=1 - mp)
    swap.start()
    place_indices(n, keep, spill, me, placer_v, local_v, state_v, sendi_v)
    loads[2].wait()
    swap.wait()

    total = sums_v[...] + sums_got[...]
    inverse = lax.rsqrt(total[0:1] / full_width + epsilon)
    coef = inverse * inverse * inverse * total[1:2] / full_width
    line = lax.broadcasted_iota(jnp.int32, (LANES, tokens), 0)
    back = jnp.where(line == 0, inverse, jnp.where(line == 1, coef, 0.0)).T
    for j in range(width // chunk):
        cols = pl.ds(j * chunk, chunk)
        norm_back = back[:, 0:1] * scaled_v[:, cols] - emb_v[:, cols].astype(jnp.float32) * back[:, 1:2]
        part = (stream_v[:, cols].astype(jnp.float32) + norm_back).astype(jnp.bfloat16)
        if spill:
            rows_v[:, cols] = part
        place_rows(j, chunk, keep, spill, placer_v, part, send_v, over_v)

    send, arrive = make_sender(
        n, pipe, other, me, send_v, sendi_v, rows_out, index_out,
        (send_sem, recv_sem, isend_sem, irecv_sem),
    )
    if spill:
        lines = n // 2
        at, beside = me // 2, partner(me, 1, n)
        pair = remote(over_v.at[other], spill_out.at[0, pipe], pair_send, pair_recv, pipe=other)
        pair.start()
        own_over = pltpu.make_async_copy(over_v.at[pipe], spill_out.at[0, pipe], own_sem.at[2])
        own_over.start()
        kept = pltpu.make_async_copy(rows_v, kept_out, own_sem.at[3])
        kept.start()

        def along(up, r, source, to):
            return remote(
                spill_out.at[partner(me, source, n)], spill_out.at[partner(to, source, n)],
                line_send.at[up, r], line_recv.at[up, r], dp=to,
            )

        def across(source):
            return remote(
                spill_out.at[partner(me, source, n)], spill_out.at[partner(beside, source, n)],
                side_send.at[source // 2], side_recv.at[source // 2], dp=beside,
            )

        def pass_on(r):
            for up in (1, 0):
                step = 2 if up else -2
                source = me - step * r
                here = (at >= r) if up else (at + r < lines)
                more = (at + 1 < lines) if up else (at >= 1)
                if r > 0:

                    @pl.when(here)
                    def _():
                        remote(
                            spill_out.at[0], spill_out.at[partner(me, source, n)],
                            line_send.at[up, r], line_recv.at[up, r], dp=beside,
                        ).wait_recv()
                        across(source).start()

                @pl.when(here & more)
                def _():
                    along(up, r + 1, source, me + step).start()

            if r == 0:
                across(me).start()

        def finish(r):
            for up in (1, 0):
                step = 2 if up else -2
                source = me - step * r
                here = (at >= r) if up else (at + r < lines)
                more = (at + 1 < lines) if up else (at >= 1)

                @pl.when(here & more)
                def _():
                    along(up, r + 1, source, me + step).wait_send()

        send(1, False)
        own_over.wait()
        pair.wait()
        pass_on(0)
        for k in range(2, n):
            send(k, False)
            if k % 2 == 1 and k // 2 < lines:
                pass_on(k // 2)
        send(0, True)
    else:

        def send_on(k, carry):
            send(k, False)
            return carry

        lax.fori_loop(1, n, send_on, 0)
        send(0, True)
    own_rows = pltpu.make_async_copy(send_v.at[0, pipe], rows_out.at[0, pipe], own_sem.at[0])
    own_index = pltpu.make_async_copy(sendi_v.at[0], index_out.at[0, pipe], own_sem.at[1])
    own_rows.start()
    own_index.start()
    lax.fori_loop(0, n, arrive, 0)
    own_rows.wait()
    own_index.wait()
    if spill:
        for r in range(lines):
            finish(r)

        def side(z, carry):
            remote(
                spill_out.at[partner(me, 2 * z, n)], spill_out.at[partner(me, 2 * z + beside % 2, n)],
                side_send.at[z], side_recv.at[z], dp=beside,
            ).wait()
            return carry

        lax.fori_loop(0, lines, side, 0)
        kept.wait()


def exchange(ids, embedded, gain, proj_grad, weight, stream, n, n_mp, cap, keep, spill, block_rows):
    tokens, width = embedded.shape
    inner = proj_grad.shape[1]
    half = width // 2
    chunk = min(256, half)
    index_width = 3 * LANES if spill else cap
    over = (spill or 16, half)
    kept = (tokens, width) if spill else (8, LANES)
    any_space = pl.BlockSpec(memory_space=pl.ANY)
    vmem = pl.BlockSpec(memory_space=pltpu.VMEM)
    dma = pltpu.SemaphoreType.DMA
    return pl.pallas_call(
        functools.partial(exchange_kernel, n, cap, keep, spill, block_rows, width * n_mp, chunk),
        out_shape=(
            jax.ShapeDtypeStruct((n, 2, keep, half), jnp.bfloat16),
            jax.ShapeDtypeStruct((n, 2, 1, index_width), jnp.int32),
            jax.ShapeDtypeStruct((n if spill else 1, 2) + over, jnp.bfloat16),
            jax.ShapeDtypeStruct(kept, jnp.bfloat16),
        ),
        in_specs=[vmem, vmem] + [any_space] * 4,
        out_specs=(any_space,) * 4,
        scratch_shapes=[
            pltpu.VMEM((tokens, width), jnp.bfloat16),
            pltpu.VMEM((tokens, inner), jnp.bfloat16),
            pltpu.VMEM((width, inner), jnp.bfloat16),
            pltpu.VMEM((tokens, width), jnp.bfloat16),
            pltpu.VMEM((tokens, width), jnp.float32),
            pltpu.VMEM((tokens, width), jnp.bfloat16),
            pltpu.VMEM((n, 2, keep, half), jnp.bfloat16),
            pltpu.VMEM((n, 1, index_width), jnp.int32),
            pltpu.VMEM((2,) + over, jnp.bfloat16),
            pltpu.VMEM((8, tokens), jnp.float32),
            pltpu.VMEM((8, tokens), jnp.float32),
            pltpu.VMEM((n * keep + (LANES if spill else 0), tokens), jnp.bfloat16),
            pltpu.VMEM((8, tokens), jnp.bfloat16),
            pltpu.VMEM((8, LANES), jnp.int32),
            dma((3,)),
            dma((width // chunk,)),
            dma,
            dma,
            dma((n, 2)),
            dma((n, 2)),
            dma((n, 2)),
            dma((n, 2)),
            dma((4,)),
            dma,
            dma,
            dma((2, n)),
            dma((2, n)),
            dma((n,)),
            dma((n,)),
        ],
        compiler_params=pltpu.CompilerParams(
            collective_id=0, has_side_effects=True, vmem_limit_bytes=VMEM_LIMIT
        ),
    )(ids, gain, embedded, proj_grad, weight, stream)


def full_kernel(
    n, cap, block_rows, ids_ref, rows_v, rows_out, index_out, send_v, sendi_v, placer_v, local_v,
    send_sem, recv_sem, isend_sem, irecv_sem, own_sem,
):
    pipe = lax.axis_index("pipe")
    me = lax.axis_index("dp")
    other = 1 - pipe
    barrier = greet_all(n, pipe, other, me, None)
    pl.semaphore_wait(barrier, 2 * n - 1)
    find_places(n, cap, 0, block_rows, me, ids_ref, placer_v, local_v, None)
    place_indices(n, cap, 0, me, placer_v, local_v, None, sendi_v)
    width = rows_v.shape[1]
    chunk = min(256, width // 2)
    for c in range(width // chunk):
        place_rows(c, chunk, cap, 0, placer_v, rows_v[:, c * chunk:(c + 1) * chunk], send_v, None)
    send, arrive = make_sender(
        n, pipe, other, me, send_v, sendi_v, rows_out, index_out,
        (send_sem, recv_sem, isend_sem, irecv_sem),
    )

    def send_on(k, carry):
        send(k, False)
        return carry

    lax.fori_loop(1, n, send_on, 0)
    send(0, True)
    own_rows = pltpu.make_async_copy(send_v.at[0, pipe], rows_out.at[0, pipe], own_sem.at[0])
    own_index = pltpu.make_async_copy(sendi_v.at[0], index_out.at[0, pipe], own_sem.at[1])
    own_rows.start()
    own_index.start()
    lax.fori_loop(0, n, arrive, 0)
    own_rows.wait()
    own_index.wait()


def full_exchange(ids, rows, n, cap, block_rows):
    tokens, width = rows.shape
    half = width // 2
    any_space = pl.BlockSpec(memory_space=pl.ANY)
    vmem = pl.BlockSpec(memory_space=pltpu.VMEM)
    dma = pltpu.SemaphoreType.DMA
    return pl.pallas_call(
        functools.partial(full_kernel, n, cap, block_rows),
        out_shape=(
            jax.ShapeDtypeStruct((n, 2, cap, half), jnp.bfloat16),
            jax.ShapeDtypeStruct((n, 2, 1, cap), jnp.int32),
        ),
        in_specs=[vmem, vmem],
        out_specs=(any_space, any_space),
        scratch_shapes=[
            pltpu.VMEM((n, 2, cap, half), jnp.bfloat16),
            pltpu.VMEM((n, 1, cap), jnp.int32),
            pltpu.VMEM((n * cap, tokens), jnp.bfloat16),
            pltpu.VMEM((8, tokens), jnp.bfloat16),
            dma((n, 2)),
            dma((n, 2)),
            dma((n, 2)),
            dma((n, 2)),
            dma((2,)),
        ],
        compiler_params=pltpu.CompilerParams(
            collective_id=1, has_side_effects=True, vmem_limit_bytes=VMEM_LIMIT
        ),
    )(ids, rows)


def table_kernel(spilled, index_ref, rows_ref, *rest):
    if spilled:
        over_ref, out_ref, wide_v = rest
    else:
        out_ref, wide_v = rest
    blocks, cap, half = rows_ref.shape
    lines = half // LANES
    pieces = 16
    while out_ref.shape[0] % (8 * pieces):
        pieces //= 2
    zero_rows = out_ref.shape[0] // pieces

    def clear(i, carry):
        out_ref[pl.ds(pl.multiple_of(i * zero_rows, 8), zero_rows), :] = jnp.zeros(
            (zero_rows, LANES), jnp.float32
        )
        return carry

    lax.fori_loop(0, pieces, clear, 0)

    def add_row(v, c):
        v = pl.multiple_of(v * lines, lines)
        out_ref[pl.ds(v, lines), :] += wide_v[pl.ds(pl.multiple_of(c * lines, lines), lines), :]

    def block(b, carry):
        for j in range(lines):
            wide_v[pl.ds(j, cap, stride=lines), :] = rows_ref[b, :, j * LANES:(j + 1) * LANES].astype(
                jnp.float32
            )

        def add(g, carry):
            for u in range(8):
                add_row(index_ref[b, 0, g * 8 + u], g * 8 + u)
            return carry

        lax.fori_loop(0, cap // 8, add, 0)
        if spilled:

            @pl.when(index_ref[b, 0, 2 * LANES + 1] > 0)
            def _():
                for j in range(lines):
                    wide_v[pl.ds(j, spilled, stride=lines), :] = over_ref[
                        b, :, j * LANES:(j + 1) * LANES
                    ].astype(
                        jnp.float32
                    )

                count = index_ref[b, 0, 2 * LANES + 1]
                start = index_ref[b, 0, 2 * LANES + 2]

                def add_spilled(g, carry):
                    for u in range(8):
                        here = g * 8 + u < count
                        c = jnp.minimum(start + g * 8 + u, spilled - 1)
                        v = pl.multiple_of(jnp.where(here, index_ref[b, 0, LANES + c], 0) * lines, lines)
                        row = wide_v[pl.ds(pl.multiple_of(c * lines, lines), lines), :]
                        out_ref[pl.ds(v, lines), :] += jnp.where(here, row, 0.0)
                    return carry

                lax.fori_loop(0, (count + 7) // 8, add_spilled, 0)

        return carry

    lax.fori_loop(0, blocks, block, 0)


def table(index, rows, over, block_rows):
    n, stacks, cap, half = rows.shape
    lines = half // LANES
    spilled = 0 if over is None else over.shape[2]
    operands = [index.reshape(n * stacks, 1, -1), rows.reshape(n * stacks, cap, half)]
    in_specs = [pl.BlockSpec(memory_space=pltpu.SMEM), pl.BlockSpec(memory_space=pltpu.VMEM)]
    scratch = [pltpu.VMEM((max(cap, spilled) * lines, LANES), jnp.float32)]
    if spilled:
        operands.append(over.reshape(n * stacks, spilled, half))
        in_specs.append(pl.BlockSpec(memory_space=pltpu.VMEM))
    return pl.pallas_call(
        functools.partial(table_kernel, spilled),
        out_shape=jax.ShapeDtypeStruct((block_rows * lines, LANES), jnp.float32),
        in_specs=in_specs,
        out_specs=pl.BlockSpec(memory_space=pltpu.VMEM),
        scratch_shapes=scratch,
        compiler_params=pltpu.CompilerParams(vmem_limit_bytes=VMEM_LIMIT),
    )(*operands)


def on_device(token_ids, embedded, norm_gain, proj_grad, proj_weight, stream_grad):
    n = lax.axis_size("dp")
    tokens = token_ids.shape[1]
    cap = max(2, 2 * tokens // n)
    block_rows = VOCAB // n
    tiers = cap % 32 == 0 and cap <= LANES
    keep = cap // 2 if tiers else cap
    spill = keep + 16 if tiers else 0
    rows, index, over, kept = exchange(
        token_ids, embedded[0], norm_gain, proj_grad[0], proj_weight[0], stream_grad[0],
        n, lax.axis_size("mp"), cap, keep, spill, block_rows,
    )
    half = rows.shape[-1]
    if tiers:

        def whole():
            full_rows, full_index = full_exchange(token_ids, kept, n, cap, block_rows)
            return table(full_index, full_rows, None, block_rows)

        def short():
            return table(index, rows, over, block_rows)

        out = lax.cond(jnp.max(index[:, :, 0, 2 * LANES]) > 0, whole, short)
    else:
        out = table(index, rows, None, block_rows)
    return out.reshape(block_rows, 1, half)


def solution(mesh):
    return jax.shard_map(
        on_device,
        mesh=mesh,
        in_specs=(
            P("pipe", "dp"),
            P("pipe", "dp", "mp"),
            P("pipe", "mp"),
            P("pipe", "dp", None),
            P("pipe", "mp", None),
            P("pipe", "dp", "mp"),
        ),
        out_specs=P("dp", "mp", "pipe"),
        check_vma=False,
    )
```

```python
import functools

import jax
import jax.numpy as jnp
from jax import lax
from jax.experimental import pallas as pl
from jax.experimental.pallas import tpu as pltpu
from jax.sharding import PartitionSpec as P

VOCAB = 32128
LANES = 128
epsilon = 1e-06
VMEM_LIMIT = 60 * 1024 * 1024


def partner(me, k, n):
    out, bit = 0, 1
    while bit < n:
        mine = (me // bit) % 2
        flip = (k // bit) % 2
        out = out + bit * (mine + flip - 2 * mine * flip)
        bit *= 2
    return out


def contract_last(a, b):
    return lax.dot_general(a, b, (((1,), (1,)), ((), ())), preferred_element_type=jnp.float32)


def greet_all(n, pipe, other, me, mp):
    barrier = pltpu.get_barrier_semaphore()

    def greet(k, carry):
        d = partner(me, k, n)
        pl.semaphore_signal(
            barrier, inc=1, device_id={"dp": d, "pipe": other}, device_id_type=pl.DeviceIdType.MESH
        )

        @pl.when(k > 0)
        def _():
            pl.semaphore_signal(
                barrier, inc=1, device_id={"dp": d, "pipe": pipe}, device_id_type=pl.DeviceIdType.MESH
            )

        return carry

    lax.fori_loop(0, n, greet, 0)
    if mp is not None:
        pl.semaphore_signal(
            barrier, inc=1, device_id={"mp": 1 - mp}, device_id_type=pl.DeviceIdType.MESH
        )
    return barrier


def find_places(n, keep, spill, block_rows, me, ids_ref, placer_v, local_v, state_v):
    tokens = ids_ref.shape[1]
    ids = ids_ref[...]
    owner = lax.broadcasted_iota(jnp.int32, (n, tokens), 0)
    owner_low = owner * block_rows
    match = (ids >= owner_low) & (ids < owner_low + block_rows)
    match_f = match.astype(jnp.float32)
    before = (
        lax.broadcasted_iota(jnp.int32, (tokens, tokens), 0)
        < lax.broadcasted_iota(jnp.int32, (tokens, tokens), 1)
    ).astype(jnp.float32).astype(jnp.bfloat16)
    rank = match_f * jnp.dot(match_f.astype(jnp.bfloat16), before, preferred_element_type=jnp.float32)
    rank = jnp.sum(rank, axis=0, keepdims=True).astype(jnp.int32)
    token_owner = jnp.sum(jnp.where(match, owner, 0), axis=0, keepdims=True)
    position = jnp.where(rank < keep, partner(me, token_owner, n) * keep + rank, -1)
    local = ids - token_owner * block_rows
    high = local // 64
    row = lax.broadcasted_iota(jnp.int32, (8, tokens), 0)
    parts = jnp.where(row == 0, high, jnp.where(row == 1, local - high * 64, 0))
    parts = jnp.where(row == 2, token_owner + 1, parts)
    local_v[...] = parts.astype(jnp.float32).astype(jnp.bfloat16)
    if spill:
        over = match_f * (rank >= keep).astype(jnp.float32)
        count = jnp.sum(over, axis=1, keepdims=True)
        start = jnp.zeros((1, 1), jnp.float32)
        begin = jnp.zeros((1, tokens), jnp.float32)
        for o in range(n):
            begin = begin + over[o:o + 1] * start
            start = start + count[o:o + 1]
        behind = n * keep + begin.astype(jnp.int32) + rank - keep
        position = jnp.where(rank >= keep, behind, position)
        full = (start > spill).astype(jnp.float32)
        state_v[1:2, :] = jnp.broadcast_to(full, (1, LANES)).astype(jnp.int32)
    slots = lax.broadcasted_iota(jnp.int32, placer_v.shape, 0)
    placer_v[...] = (position == slots).astype(jnp.float32).astype(jnp.bfloat16)


def place_indices(n, keep, spill, me, placer_v, local_v, state_v, sendi_v):
    parts = contract_last(local_v[...], placer_v[...])
    found = (parts[0:1] * 64.0 + parts[1:2]).astype(jnp.int32)
    if spill:
        state_v[0:1, :] = found[:, n * keep:]
        state_v[2:3, :] = parts[2:3, n * keep:].astype(jnp.int32)
        lane = lax.broadcasted_iota(jnp.int32, (1, LANES), 1)
        sendi_v[...] = jnp.zeros(sendi_v.shape, jnp.int32)
    for k in range(n):
        sendi_v[k, :, 0:keep] = found[:, k * keep:(k + 1) * keep]
        if spill:
            d = partner(me, k, n)
            there = state_v[2:3, :]
            count = jnp.sum(((there == d + 1) & (lane < spill)).astype(jnp.float32), axis=1, keepdims=True)
            start = jnp.sum(((there > 0) & (there < d + 1)).astype(jnp.float32), axis=1, keepdims=True)
            facts = jnp.where(lane == 1, count, start).astype(jnp.int32)
            sendi_v[k, :, LANES:2 * LANES] = state_v[0:1, :]
            sendi_v[k, :, 2 * LANES:] = jnp.where(lane == 0, state_v[1:2, :], facts)


def place_rows(c, chunk, keep, spill, placer_v, part, send_v, over_v):
    n, _, _, half = send_v.shape
    p, cols = c * chunk // half, pl.ds(c * chunk % half, chunk)
    placed = jnp.dot(
        placer_v[0:n * keep + spill, :], part, preferred_element_type=jnp.float32
    ).astype(jnp.bfloat16)
    send_v[:, p, :, cols] = placed[:n * keep].reshape(n, keep, chunk)
    if spill:
        over_v[p, :, cols] = placed[n * keep:]


def remote(src, dst, send_sem, recv_sem, **where):
    return pltpu.make_async_remote_copy(
        src_ref=src, dst_ref=dst, send_sem=send_sem, recv_sem=recv_sem,
        device_id=where, device_id_type=pl.DeviceIdType.MESH,
    )


def make_sender(n, pipe, other, me, send_v, sendi_v, rows_out, index_out, sems):
    send_sem, recv_sem, isend_sem, irecv_sem = sems

    def copies(k, p, s):
        d = partner(me, k, n)
        return (
            remote(send_v.at[k, p], rows_out.at[k, s], send_sem.at[k, p], recv_sem.at[k, s], dp=d, pipe=p),
            remote(sendi_v.at[k], index_out.at[k, s], isend_sem.at[k, p], irecv_sem.at[k, s], dp=d, pipe=p),
        )

    def send(k, own_chip):
        for copy in copies(k, other, pipe):
            copy.start()
        if not own_chip:
            for copy in copies(k, pipe, pipe):
                copy.start()

    def arrive(k, carry):
        for copy in copies(k, other, pipe):
            copy.wait_send()
        for copy in copies(k, other, other):
            copy.wait_recv()

        @pl.when(k > 0)
        def _():
            for copy in copies(k, pipe, pipe):
                copy.wait_send()
            for copy in copies(k, other, pipe):
                copy.wait_recv()

        return carry

    return send, arrive


def exchange_kernel(
    n, cap, keep, spill, block_rows, full_width, chunk,
    ids_ref, gain_ref, embedded, proj_grad, weight, stream,
    rows_out, index_out, spill_out, kept_out,
    emb_v, grad_v, weight_v, stream_v, scaled_v, rows_v, send_v, sendi_v, over_v, sums_v, sums_got,
    placer_v, local_v, state_v,
    in_sem, weight_sem, sum_send, sum_recv, send_sem, recv_sem, isend_sem, irecv_sem, own_sem,
    pair_send, pair_recv, line_send, line_recv, side_send, side_recv,
):
    pipe = lax.axis_index("pipe")
    me = lax.axis_index("dp")
    mp = lax.axis_index("mp")
    other = 1 - pipe
    tokens, width = emb_v.shape
    half = width // 2

    loads = [
        pltpu.make_async_copy(proj_grad, grad_v, in_sem.at[0]),
        pltpu.make_async_copy(embedded, emb_v, in_sem.at[1]),
        pltpu.make_async_copy(stream, stream_v, in_sem.at[2]),
    ]
    chunks = [
        pltpu.make_async_copy(
            weight.at[pl.ds(j * chunk, chunk)], weight_v.at[pl.ds(j * chunk, chunk)], weight_sem.at[j]
        )
        for j in range(width // chunk)
    ]
    loads[0].start()
    chunks[0].start()
    loads[1].start()
    for copy in chunks[1:]:
        copy.start()
    loads[2].start()
    barrier = greet_all(n, pipe, other, me, mp)
    find_places(n, keep, spill, block_rows, me, ids_ref, placer_v, local_v, state_v)

    loads[0].wait()
    mixed = jnp.zeros((tokens, 1), jnp.float32)
    square = jnp.zeros((tokens, 1), jnp.float32)
    for j in range(width // chunk):
        cols = pl.ds(j * chunk, chunk)
        chunks[j].wait()
        if j == 0:
            loads[1].wait()
        scaled = contract_last(grad_v[...], weight_v[cols, :]) * gain_ref[:, cols]
        scaled_v[:, cols] = scaled
        inputs = emb_v[:, cols].astype(jnp.float32)
        square = square + jnp.sum(inputs * inputs, axis=1, keepdims=True)
        mixed = mixed + jnp.sum(inputs * scaled, axis=1, keepdims=True)
    lane = lax.broadcasted_iota(jnp.int32, (tokens, LANES), 1)
    packed = jnp.where(lane == 0, square, jnp.where(lane == 1, mixed, 0.0))
    sums_v[...] = packed.T[:8]

    pl.semaphore_wait(barrier, 2 * n)
    swap = remote(sums_v, sums_got, sum_send, sum_recv, mp=1 - mp)
    swap.start()
    place_indices(n, keep, spill, me, placer_v, local_v, state_v, sendi_v)
    loads[2].wait()
    swap.wait()

    total = sums_v[...] + sums_got[...]
    inverse = lax.rsqrt(total[0:1] / full_width + epsilon)
    coef = inverse * inverse * inverse * total[1:2] / full_width
    line = lax.broadcasted_iota(jnp.int32, (LANES, tokens), 0)
    back = jnp.where(line == 0, inverse, jnp.where(line == 1, coef, 0.0)).T
    for j in range(width // chunk):
        cols = pl.ds(j * chunk, chunk)
        norm_back = back[:, 0:1] * scaled_v[:, cols] - emb_v[:, cols].astype(jnp.float32) * back[:, 1:2]
        part = (stream_v[:, cols].astype(jnp.float32) + norm_back).astype(jnp.bfloat16)
        if spill:
            rows_v[:, cols] = part
        place_rows(j, chunk, keep, spill, placer_v, part, send_v, over_v)

    send, arrive = make_sender(
        n, pipe, other, me, send_v, sendi_v, rows_out, index_out,
        (send_sem, recv_sem, isend_sem, irecv_sem),
    )
    if spill:
        lines = n // 2
        at, beside = me // 2, partner(me, 1, n)
        pair = remote(over_v.at[other], spill_out.at[0, pipe], pair_send, pair_recv, pipe=other)
        pair.start()
        own_over = pltpu.make_async_copy(over_v.at[pipe], spill_out.at[0, pipe], own_sem.at[2])
        own_over.start()
        kept = pltpu.make_async_copy(rows_v, kept_out, own_sem.at[3])
        kept.start()

        def along(up, r, source, to):
            return remote(
                spill_out.at[partner(me, source, n)], spill_out.at[partner(to, source, n)],
                line_send.at[up, r], line_recv.at[up, r], dp=to,
            )

        def across(source):
            return remote(
                spill_out.at[partner(me, source, n)], spill_out.at[partner(beside, source, n)],
                side_send.at[source // 2], side_recv.at[source // 2], dp=beside,
            )

        def pass_on(r):
            for up in (1, 0):
                step = 2 if up else -2
                source = me - step * r
                here = (at >= r) if up else (at + r < lines)
                more = (at + 1 < lines) if up else (at >= 1)
                if r > 0:

                    @pl.when(here)
                    def _():
                        remote(
                            spill_out.at[0], spill_out.at[partner(me, source, n)],
                            line_send.at[up, r], line_recv.at[up, r], dp=beside,
                        ).wait_recv()
                        across(source).start()

                @pl.when(here & more)
                def _():
                    along(up, r + 1, source, me + step).start()

            if r == 0:
                across(me).start()

        def finish(r):
            for up in (1, 0):
                step = 2 if up else -2
                source = me - step * r
                here = (at >= r) if up else (at + r < lines)
                more = (at + 1 < lines) if up else (at >= 1)

                @pl.when(here & more)
                def _():
                    along(up, r + 1, source, me + step).wait_send()

        send(1, False)
        own_over.wait()
        pair.wait()
        pass_on(0)
        for k in range(2, n, 2):
            send(k, False)
            pass_on(k // 2)
        for k in range(3, n, 2):
            send(k, False)
        send(0, True)
    else:

        def send_on(k, carry):
            send(k, False)
            return carry

        lax.fori_loop(1, n, send_on, 0)
        send(0, True)
    own_rows = pltpu.make_async_copy(send_v.at[0, pipe], rows_out.at[0, pipe], own_sem.at[0])
    own_index = pltpu.make_async_copy(sendi_v.at[0], index_out.at[0, pipe], own_sem.at[1])
    own_rows.start()
    own_index.start()
    lax.fori_loop(0, n, arrive, 0)
    own_rows.wait()
    own_index.wait()
    if spill:
        for r in range(lines):
            finish(r)

        def side(z, carry):
            remote(
                spill_out.at[partner(me, 2 * z, n)], spill_out.at[partner(me, 2 * z + beside % 2, n)],
                side_send.at[z], side_recv.at[z], dp=beside,
            ).wait()
            return carry

        lax.fori_loop(0, lines, side, 0)
        kept.wait()


def exchange(ids, embedded, gain, proj_grad, weight, stream, n, n_mp, cap, keep, spill, block_rows):
    tokens, width = embedded.shape
    inner = proj_grad.shape[1]
    half = width // 2
    chunk = min(256, half)
    index_width = 3 * LANES if spill else cap
    over = (spill or 16, half)
    kept = (tokens, width) if spill else (8, LANES)
    any_space = pl.BlockSpec(memory_space=pl.ANY)
    vmem = pl.BlockSpec(memory_space=pltpu.VMEM)
    dma = pltpu.SemaphoreType.DMA
    return pl.pallas_call(
        functools.partial(exchange_kernel, n, cap, keep, spill, block_rows, width * n_mp, chunk),
        out_shape=(
            jax.ShapeDtypeStruct((n, 2, keep, half), jnp.bfloat16),
            jax.ShapeDtypeStruct((n, 2, 1, index_width), jnp.int32),
            jax.ShapeDtypeStruct((n if spill else 1, 2) + over, jnp.bfloat16),
            jax.ShapeDtypeStruct(kept, jnp.bfloat16),
        ),
        in_specs=[vmem, vmem] + [any_space] * 4,
        out_specs=(any_space,) * 4,
        scratch_shapes=[
            pltpu.VMEM((tokens, width), jnp.bfloat16),
            pltpu.VMEM((tokens, inner), jnp.bfloat16),
            pltpu.VMEM((width, inner), jnp.bfloat16),
            pltpu.VMEM((tokens, width), jnp.bfloat16),
            pltpu.VMEM((tokens, width), jnp.float32),
            pltpu.VMEM((tokens, width), jnp.bfloat16),
            pltpu.VMEM((n, 2, keep, half), jnp.bfloat16),
            pltpu.VMEM((n, 1, index_width), jnp.int32),
            pltpu.VMEM((2,) + over, jnp.bfloat16),
            pltpu.VMEM((8, tokens), jnp.float32),
            pltpu.VMEM((8, tokens), jnp.float32),
            pltpu.VMEM((n * keep + (LANES if spill else 0), tokens), jnp.bfloat16),
            pltpu.VMEM((8, tokens), jnp.bfloat16),
            pltpu.VMEM((8, LANES), jnp.int32),
            dma((3,)),
            dma((width // chunk,)),
            dma,
            dma,
            dma((n, 2)),
            dma((n, 2)),
            dma((n, 2)),
            dma((n, 2)),
            dma((4,)),
            dma,
            dma,
            dma((2, n)),
            dma((2, n)),
            dma((n,)),
            dma((n,)),
        ],
        compiler_params=pltpu.CompilerParams(
            collective_id=0, has_side_effects=True, vmem_limit_bytes=VMEM_LIMIT
        ),
    )(ids, gain, embedded, proj_grad, weight, stream)


def full_kernel(
    n, cap, block_rows, ids_ref, rows_v, rows_out, index_out, send_v, sendi_v, placer_v, local_v,
    send_sem, recv_sem, isend_sem, irecv_sem, own_sem,
):
    pipe = lax.axis_index("pipe")
    me = lax.axis_index("dp")
    other = 1 - pipe
    barrier = greet_all(n, pipe, other, me, None)
    pl.semaphore_wait(barrier, 2 * n - 1)
    find_places(n, cap, 0, block_rows, me, ids_ref, placer_v, local_v, None)
    place_indices(n, cap, 0, me, placer_v, local_v, None, sendi_v)
    width = rows_v.shape[1]
    chunk = min(256, width // 2)
    for c in range(width // chunk):
        place_rows(c, chunk, cap, 0, placer_v, rows_v[:, c * chunk:(c + 1) * chunk], send_v, None)
    send, arrive = make_sender(
        n, pipe, other, me, send_v, sendi_v, rows_out, index_out,
        (send_sem, recv_sem, isend_sem, irecv_sem),
    )

    def send_on(k, carry):
        send(k, False)
        return carry

    lax.fori_loop(1, n, send_on, 0)
    send(0, True)
    own_rows = pltpu.make_async_copy(send_v.at[0, pipe], rows_out.at[0, pipe], own_sem.at[0])
    own_index = pltpu.make_async_copy(sendi_v.at[0], index_out.at[0, pipe], own_sem.at[1])
    own_rows.start()
    own_index.start()
    lax.fori_loop(0, n, arrive, 0)
    own_rows.wait()
    own_index.wait()


def full_exchange(ids, rows, n, cap, block_rows):
    tokens, width = rows.shape
    half = width // 2
    any_space = pl.BlockSpec(memory_space=pl.ANY)
    vmem = pl.BlockSpec(memory_space=pltpu.VMEM)
    dma = pltpu.SemaphoreType.DMA
    return pl.pallas_call(
        functools.partial(full_kernel, n, cap, block_rows),
        out_shape=(
            jax.ShapeDtypeStruct((n, 2, cap, half), jnp.bfloat16),
            jax.ShapeDtypeStruct((n, 2, 1, cap), jnp.int32),
        ),
        in_specs=[vmem, vmem],
        out_specs=(any_space, any_space),
        scratch_shapes=[
            pltpu.VMEM((n, 2, cap, half), jnp.bfloat16),
            pltpu.VMEM((n, 1, cap), jnp.int32),
            pltpu.VMEM((n * cap, tokens), jnp.bfloat16),
            pltpu.VMEM((8, tokens), jnp.bfloat16),
            dma((n, 2)),
            dma((n, 2)),
            dma((n, 2)),
            dma((n, 2)),
            dma((2,)),
        ],
        compiler_params=pltpu.CompilerParams(
            collective_id=1, has_side_effects=True, vmem_limit_bytes=VMEM_LIMIT
        ),
    )(ids, rows)


def table_kernel(spilled, index_ref, rows_ref, *rest):
    if spilled:
        over_ref, out_ref, wide_v = rest
    else:
        out_ref, wide_v = rest
    blocks, cap, half = rows_ref.shape
    lines = half // LANES
    pieces = 16
    while out_ref.shape[0] % (8 * pieces):
        pieces //= 2
    zero_rows = out_ref.shape[0] // pieces

    def clear(i, carry):
        out_ref[pl.ds(pl.multiple_of(i * zero_rows, 8), zero_rows), :] = jnp.zeros(
            (zero_rows, LANES), jnp.float32
        )
        return carry

    lax.fori_loop(0, pieces, clear, 0)

    def add_row(v, c):
        v = pl.multiple_of(v * lines, lines)
        out_ref[pl.ds(v, lines), :] += wide_v[pl.ds(pl.multiple_of(c * lines, lines), lines), :]

    def block(b, carry):
        for j in range(lines):
            wide_v[pl.ds(j, cap, stride=lines), :] = rows_ref[b, :, j * LANES:(j + 1) * LANES].astype(
                jnp.float32
            )

        def add(g, carry):
            for u in range(8):
                add_row(index_ref[b, 0, g * 8 + u], g * 8 + u)
            return carry

        lax.fori_loop(0, cap // 8, add, 0)
        if spilled:

            @pl.when(index_ref[b, 0, 2 * LANES + 1] > 0)
            def _():
                for j in range(lines):
                    wide_v[pl.ds(j, spilled, stride=lines), :] = over_ref[
                        b, :, j * LANES:(j + 1) * LANES
                    ].astype(
                        jnp.float32
                    )

                count = index_ref[b, 0, 2 * LANES + 1]
                start = index_ref[b, 0, 2 * LANES + 2]

                def add_spilled(g, carry):
                    for u in range(8):
                        here = g * 8 + u < count
                        c = jnp.minimum(start + g * 8 + u, spilled - 1)
                        v = pl.multiple_of(jnp.where(here, index_ref[b, 0, LANES + c], 0) * lines, lines)
                        row = wide_v[pl.ds(pl.multiple_of(c * lines, lines), lines), :]
                        out_ref[pl.ds(v, lines), :] += jnp.where(here, row, 0.0)
                    return carry

                lax.fori_loop(0, (count + 7) // 8, add_spilled, 0)

        return carry

    lax.fori_loop(0, blocks, block, 0)


def table(index, rows, over, block_rows):
    n, stacks, cap, half = rows.shape
    lines = half // LANES
    spilled = 0 if over is None else over.shape[2]
    operands = [index.reshape(n * stacks, 1, -1), rows.reshape(n * stacks, cap, half)]
    in_specs = [pl.BlockSpec(memory_space=pltpu.SMEM), pl.BlockSpec(memory_space=pltpu.VMEM)]
    scratch = [pltpu.VMEM((max(cap, spilled) * lines, LANES), jnp.float32)]
    if spilled:
        operands.append(over.reshape(n * stacks, spilled, half))
        in_specs.append(pl.BlockSpec(memory_space=pltpu.VMEM))
    return pl.pallas_call(
        functools.partial(table_kernel, spilled),
        out_shape=jax.ShapeDtypeStruct((block_rows * lines, LANES), jnp.float32),
        in_specs=in_specs,
        out_specs=pl.BlockSpec(memory_space=pltpu.VMEM),
        scratch_shapes=scratch,
        compiler_params=pltpu.CompilerParams(vmem_limit_bytes=VMEM_LIMIT),
    )(*operands)


def on_device(token_ids, embedded, norm_gain, proj_grad, proj_weight, stream_grad):
    n = lax.axis_size("dp")
    tokens = token_ids.shape[1]
    cap = max(2, 2 * tokens // n)
    block_rows = VOCAB // n
    tiers = cap % 32 == 0 and cap <= LANES
    keep = cap // 2 if tiers else cap
    spill = keep + 16 if tiers else 0
    rows, index, over, kept = exchange(
        token_ids, embedded[0], norm_gain, proj_grad[0], proj_weight[0], stream_grad[0],
        n, lax.axis_size("mp"), cap, keep, spill, block_rows,
    )
    half = rows.shape[-1]
    if tiers:

        def whole():
            full_rows, full_index = full_exchange(token_ids, kept, n, cap, block_rows)
            return table(full_index, full_rows, None, block_rows)

        def short():
            return table(index, rows, over, block_rows)

        out = lax.cond(jnp.max(index[:, :, 0, 2 * LANES]) > 0, whole, short)
    else:
        out = table(index, rows, None, block_rows)
    return out.reshape(block_rows, 1, half)


def solution(mesh):
    return jax.shard_map(
        on_device,
        mesh=mesh,
        in_specs=(
            P("pipe", "dp"),
            P("pipe", "dp", "mp"),
            P("pipe", "mp"),
            P("pipe", "dp", None),
            P("pipe", "mp", None),
            P("pipe", "dp", "mp"),
        ),
        out_specs=P("dp", "mp", "pipe"),
        check_vma=False,
    )
```
